256 devices in a mesh: grp: 8 (over z_lo, y), dev: 32 (over z_hi, x, core).
Axes of the slice: x: 4, y: 4, z: 8 (z_hi: 4, z_lo: 2; z = z_hi * 2 + z_lo), core: 2. Of those that a mesh axis runs over, the one named last changes fastest.
Arguments:
- patch_features: bfloat16 [1024, 360448], P(None, ('grp', 'dev')), may hold values from -12 to 12
- upstream: bfloat16 [1024, 1024], P(('grp', 'dev')), may hold values from -115200 to 115200
Outputs:
- feature_grad: bfloat16 [1024, 360448], P(None, ('grp', 'dev'))
The draws below stay inside these ranges and needn't reach their ends.
All inputs are finite; a program needn't handle non-finite values.
Results may differ from the reference program's by a relative error of at most 0.0051.
Values may be sent and summed in bfloat16 or wider, within the bound.
A program may use at most 64 MiB of HBM per device.

```python
import math
import jax
import jax.numpy as jnp
from jax import lax

WIDTH = 1408
FRAMES = 1024
PATCHES = 256
FEATURES = 360448


def draw_patch_features(key, part):
    key_base = jax.random.fold_in(key, 0)
    columns = PATCHES * WIDTH
    features = jnp.clip(jax.random.normal(key_base, (FRAMES, columns), jnp.float32), -6.0, 6.0)
    return features.astype(jnp.bfloat16)


def level_of(own_key, dims, pieces, low, top_value):
    factor_of, own = 1.0, jax.random.fold_in(own_key, 6)
    for position, parts in pieces:
        draws = jnp.exp(jax.random.uniform(jax.random.fold_in(own, position), (parts,), jnp.float32, low / len(pieces), top_value / len(pieces)))
        factor_of = factor_of * jnp.repeat(draws, dims[position] // parts).reshape([-1 if axis == position else 1 for axis in range(len(dims))])
    return factor_of


def gaussian(stream_key, dims, scale, limit, cuts=(), kind=jnp.bfloat16):
    drawn = jax.random.normal(stream_key, dims, jnp.float32) * scale
    if len(cuts) > 0:
        drawn = level_of(stream_key, dims, cuts, -0.22, 0.18) * drawn
    return jnp.clip(drawn, min=-limit, max=limit).astype(kind)


def setup_inputs(seed: int = 0) -> dict:
    keys = jax.random.split(jax.random.key(seed), 3)
    patch_features = draw_patch_features(jax.random.fold_in(keys[2], 71), 0)
    upstream = gaussian(keys[1], (FRAMES, FRAMES), ((FRAMES * FEATURES) ** 0.5), 115200.0, ((0, 256),))
    return dict(patch_features=patch_features, upstream=upstream)


def reference(patch_features, upstream):
    frames = patch_features.shape[0]
    scaling = 1.0 / math.sqrt(patch_features.shape[1])
    products = jnp.dot(patch_features, patch_features.T, preferred_element_type=jnp.float32) * scaling
    diagonal = jnp.arange(frames)[:, None] == jnp.arange(frames)[None, :]
    scores = jnp.where(diagonal, -jnp.inf, products)
    row_max = lax.optimization_barrier(jnp.max(scores, axis=1, keepdims=True))
    exponent = jnp.exp(scores - row_max)
    weights = exponent / lax.optimization_barrier(jnp.sum(exponent, axis=1, keepdims=True))
    upstream_f = upstream.astype(jnp.float32)
    weighted = lax.optimization_barrier(jnp.sum(upstream_f * weights, axis=1, keepdims=True))
    score_grad = (scaling * weights * (upstream_f - weighted)).astype(jnp.bfloat16)
    forward_part = jnp.dot(score_grad, patch_features, preferred_element_type=jnp.float32)
    backward_part = jnp.dot(score_grad.T, patch_features, preferred_element_type=jnp.float32)
    return (forward_part + backward_part).astype(jnp.bfloat16)
```

```python
import functools
import math

import jax
import jax.numpy as jnp
from jax import lax
from jax.experimental import pallas as pl
from jax.experimental.pallas import tpu as pltpu
from jax.sharding import PartitionSpec as P

MESH = pl.DeviceIdType.MESH
WIRE = jnp.float32

NY, NX, NZ, NZL, NZH, CORES = 4, 4, 8, 2, 4, 2
NXY = NX * NY
CHIP_ROWS = 8
FRAMES = 1024
HALF = FRAMES // CORES
COLS_A = 384
COLS_B = HALF - COLS_A
BLOCK = 128


def comm_kernel(
    scale,
    p_ref,
    u_ref,
    w_ref,
    xs,
    xr,
    sa,
    ra,
    sb,
    rb,
    sa2,
    ra2,
    sb2,
    rb2,
    hs,
    hr,
    ub,
    ga1,
    gb1,
    ga,
    gb,
    sg,
    x_send, x_recv, a_send, a_recv, b_send, b_recv,
    a2_send, a2_recv, b2_send, b2_recv, h_sem, u_sem,
    ga1_send, ga1_recv, gb1_send, gb1_recv,
    ga_send, ga_recv, gb_send, gb_recv,
    fa_send, fa_recv, fb_send, fb_recv,
):
    g = lax.axis_index("grp")
    d = lax.axis_index("dev")
    z_lo, y = lax.div(g, NY), lax.rem(g, NY)
    core = lax.rem(d, CORES)
    x = lax.rem(lax.div(d, CORES), NX)
    z_hi = lax.div(d, CORES * NX)
    z = z_hi * NZL + z_lo
    my_xy = y * NX + x
    my_z = z_lo * NZH + z_hi
    partner = (g, d + 1 - 2 * core)

    def at_xy(yt, xt):
        return (z_lo * NY + yt, (z_hi * NX + xt) * CORES + core)

    def z_member(dz):
        zt = lax.rem(z + dz, NZ)
        return lax.rem(zt, NZL) * NZH + lax.div(zt, NZL)

    def at_z(dz):
        zt = lax.rem(z + dz, NZ)
        return (
            lax.rem(zt, NZL) * NY + y,
            (lax.div(zt, NZL) * NX + x) * CORES + core,
        )

    def xy_offset(k):
        return lax.rem(y + k // NX, NY), lax.rem(x + k % NX, NX)

    def remote(src, dst, send, recv, to):
        return pltpu.make_async_remote_copy(
            src_ref=src, dst_ref=dst, send_sem=send, recv_sem=recv,
            device_id=to, device_id_type=MESH,
        )

    barrier = pltpu.get_barrier_semaphore()
    pl.semaphore_signal(barrier, inc=1, device_id=partner, device_id_type=MESH)
    for k in range(1, NXY):
        pl.semaphore_signal(barrier, inc=1, device_id=at_xy(*xy_offset(k)), device_id_type=MESH)
    for dz in range(1, NZ):
        pl.semaphore_signal(barrier, inc=1, device_id=at_z(dz), device_id_type=MESH)

    theirs = pl.multiple_of((1 - core) * HALF, HALF)
    mine = pl.multiple_of(core * HALF, HALF)

    def product(row0, col0):
        return lax.dot_general(
            p_ref[pl.ds(row0, BLOCK), :],
            p_ref[pl.ds(col0, HALF), :],
            (((1,), (1,)), ((), ())),
            preferred_element_type=jnp.float32,
        )

    def order(i):
        yt = lax.rem(y + 1 + lax.div(i, NZL), NY)
        return lax.rem(i, NZL) * NY + yt

    def partner_order(i):
        return order(i)

    xs[0] = product(pl.multiple_of(partner_order(0) * BLOCK, BLOCK), theirs)
    pl.semaphore_wait(barrier, 1 + (NXY - 1) + (NZ - 1))
    u_copy = remote(u_ref, ub.at[core], u_sem.at[0], u_sem.at[1], partner)
    u_copy.start()
    ub[core] = u_ref[...]

    def x_copy(i):
        return remote(xs.at[i], xr.at[i], x_send.at[i], x_recv.at[i], partner)

    x_copy(0).start()

    @pl.loop(1, 8)
    def _(i):
        xs[i] = product(pl.multiple_of(partner_order(i) * BLOCK, BLOCK), theirs)
        x_copy(i).start()

    def a_copy(k, yt, xt):
        return remote(
            sa.at[yt * NX + xt], ra.at[k], a_send.at[k], a_recv.at[k], at_xy(yt, xt)
        )

    @pl.loop(0, 8)
    def _(i):
        block = order(i)
        zl, yt = lax.div(block, NY), lax.rem(block, NY)
        own = product(pl.multiple_of(block * BLOCK, BLOCK), mine)
        x_copy(i).wait_recv()
        total = (own + xr[i]).astype(WIRE)
        for zh in range(NZH):
            for xx in range(NX):
                piece = total[(zh * NX + xx) * CHIP_ROWS : (zh * NX + xx + 1) * CHIP_ROWS]
                sa[yt * NX + xx, zl * NZH + zh] = piece[:, :COLS_A]
                sb[zl * NZH + zh, yt * NX + xx] = piece[:, COLS_A:]

        @pl.when(lax.rem(i, NZL) == NZL - 1)
        def _():
            step = lax.div(i, NZL)
            for dx in range(NX):
                xt = lax.rem(x + dx, NX)

                @pl.when(jnp.logical_or(step < NY - 1, dx > 0))
                def _():
                    a_copy(step * NX + dx, yt, xt).start()

    def b_copy(dz):
        return remote(
            sb.at[z_member(dz)], rb.at[dz], b_send.at[dz], b_recv.at[dz], at_z(dz)
        )

    for dz in range(1, NZ):
        b_copy(dz).start()

    own_slot = (NY - 1) * NX
    a_slots = [k for k in range(NXY) if k != own_slot]
    for k in a_slots:
        a_copy(k, y, x).wait_recv()

    for zz in range(NZ):
        acc = sa[my_xy, zz].astype(jnp.float32)
        for k in a_slots:
            acc = acc + ra[k, zz].astype(jnp.float32)
        sa2[zz] = acc

    def a2_copy(dz):
        return remote(
            sa2.at[z_member(dz)], ra2.at[dz], a2_send.at[dz], a2_recv.at[dz], at_z(dz)
        )

    for dz in range(1, NZ):
        a2_copy(dz).start()

    for dz in range(1, NZ):
        b_copy(dz).wait_recv()

    for m in range(NXY):
        acc = sb[my_z, m].astype(jnp.float32)
        for dz in range(1, NZ):
            acc = acc + rb[dz, m].astype(jnp.float32)
        sb2[m] = acc

    def b2_copy(k):
        yt, xt = xy_offset(k)
        return remote(
            sb2.at[yt * NX + xt], rb2.at[k], b2_send.at[k], b2_recv.at[k], at_xy(yt, xt)
        )

    for k in range(1, NXY):
        b2_copy(k).start()

    for dz in range(1, NZ):
        a2_copy(dz).wait_recv()
    acc = sa2[my_z]
    for dz in range(1, NZ):
        acc = acc + ra2[dz]
    hs[:, :COLS_A] = acc
    for k in range(1, NXY):
        b2_copy(k).wait_recv()
    acc = sb2[my_xy]
    for k in range(1, NXY):
        acc = acc + rb2[k]
    hs[:, COLS_A:] = acc

    h_copy = remote(hs, hr, h_sem.at[0], h_sem.at[1], partner)
    h_copy.start()
    u_copy.wait_recv()
    h_copy.wait_recv()

    first = core == 0
    left = jnp.where(first, hs[...], hr[...])
    right = jnp.where(first, hr[...], hs[...])
    products = jnp.concatenate([left, right], axis=1)
    row0 = (((z_lo * NY + y) * NZH + z_hi) * NX + x) * CHIP_ROWS
    row_ids = row0 + lax.broadcasted_iota(jnp.int32, (CHIP_ROWS, FRAMES), 0)
    col_ids = lax.broadcasted_iota(jnp.int32, (CHIP_ROWS, FRAMES), 1)
    scores = jnp.where(row_ids == col_ids, -jnp.inf, products * scale)
    row_max = jnp.max(scores, axis=1, keepdims=True)
    exponent = jnp.exp(scores - row_max)
    weights = exponent / jnp.sum(exponent, axis=1, keepdims=True)
    up = jnp.concatenate(
        [ub[0].astype(jnp.float32), ub[1].astype(jnp.float32)], axis=0
    )
    weighted = jnp.sum(up * weights, axis=1, keepdims=True)
    score_grad = scale * weights * (up - weighted)
    own_cols = jnp.where(first, score_grad[:, :HALF], score_grad[:, HALF:])
    own_cols = own_cols.astype(jnp.bfloat16)
    ga1[my_z] = own_cols[:, :COLS_A]
    gb1[my_xy] = own_cols[:, COLS_A:]

    def ga1_copy(dz):
        return remote(
            ga1.at[my_z], ga1.at[my_z], ga1_send.at[dz], ga1_recv.at[dz], at_z(dz)
        )

    def gb1_copy(k):
        return remote(
            gb1.at[my_xy], gb1.at[my_xy], gb1_send.at[k], gb1_recv.at[k], at_xy(*xy_offset(k))
        )

    for k in range(1, NXY):
        gb1_copy(k).start()
    for dz in range(1, NZ):
        ga1_copy(dz).start()

    def ga_copy(k):
        return remote(
            ga1, ga.at[core, my_xy], ga_send.at[k], ga_recv.at[k], at_xy(*xy_offset(k))
        )

    def gb_copy(dz):
        return remote(
            gb1, gb.at[core, my_z], gb_send.at[dz], gb_recv.at[dz], at_z(dz)
        )

    def fa_copy(k):
        yt, xt = lax.rem(y + NY - k // NX, NY), lax.rem(x + NX - k % NX, NX)
        slot = ga.at[core, yt * NX + xt]
        return remote(slot, slot, fa_send.at[k], fa_recv.at[k], partner)

    def fb_copy(dz):
        slot = gb.at[core, z_member(NZ - dz)]
        return remote(slot, slot, fb_send.at[dz], fb_recv.at[dz], partner)

    for dz in range(1, NZ):
        ga1_copy(dz).wait_recv()
    for k in range(1, NXY):
        ga_copy(k).start()
    for k in range(1, NXY):
        gb1_copy(k).wait_recv()
    for dz in range(1, NZ):
        gb_copy(dz).start()
    ga[core, my_xy] = ga1[...]
    fa_copy(0).start()
    gb[core, my_z] = gb1[...]
    fb_copy(0).start()
    for k in range(1, NXY):
        ga_copy(k).wait_recv()
        fa_copy(k).start()
    for dz in range(1, NZ):
        gb_copy(dz).wait_recv()
        fb_copy(dz).start()
    for k in range(NXY):
        fa_copy(k).wait_recv()
    for dz in range(NZ):
        fb_copy(dz).wait_recv()

    @pl.loop(0, NZL * NY)
    def _(block):
        zl, yt = lax.div(block, NY), lax.rem(block, NY)
        for zh in range(NZH):
            for xx in range(NX):
                rows = pl.ds(
                    pl.multiple_of(block * BLOCK + (zh * NX + xx) * CHIP_ROWS, CHIP_ROWS),
                    CHIP_ROWS,
                )
                for c in range(CORES):
                    sg[rows, c * HALF : c * HALF + COLS_A] = ga[
                        c, yt * NX + xx, zl * NZH + zh
                    ].astype(jnp.float32)
                    sg[rows, c * HALF + COLS_A : (c + 1) * HALF] = gb[
                        c, zl * NZH + zh, yt * NX + xx
                    ].astype(jnp.float32)

    @pl.loop(0, 8)
    def _(bi):
        ri = pl.ds(pl.multiple_of(bi * BLOCK, BLOCK), BLOCK)
        for bj in range(8):
            cj = pl.ds(bj * BLOCK, BLOCK)
            w_ref[ri, cj] = (sg[ri, cj] + sg[cj, ri].T).astype(jnp.bfloat16)

    u_copy.wait_send()
    h_copy.wait_send()
    for i in range(8):
        x_copy(i).wait_send()
    for k in a_slots:
        a_copy(k, y, x).wait_send()
    for k in range(1, NXY):
        b2_copy(k).wait_send()
        gb1_copy(k).wait_send()
        ga_copy(k).wait_send()
    for dz in range(1, NZ):
        b_copy(dz).wait_send()
        a2_copy(dz).wait_send()
        ga1_copy(dz).wait_send()
        gb_copy(dz).wait_send()
    for k in range(NXY):
        fa_copy(k).wait_send()
    for dz in range(NZ):
        fb_copy(dz).wait_send()


def grad_weights(patch_features, upstream, scale):
    dma = lambda n: pltpu.SemaphoreType.DMA((n,))
    f32, bf16 = jnp.float32, jnp.bfloat16
    return pl.pallas_call(
        functools.partial(comm_kernel, scale),
        out_shape=jax.ShapeDtypeStruct((FRAMES, FRAMES), bf16),
        in_specs=[pl.BlockSpec(memory_space=pltpu.VMEM)] * 2,
        out_specs=pl.BlockSpec(memory_space=pltpu.VMEM),
        scratch_shapes=[
            pltpu.VMEM((8, BLOCK, HALF), f32),
            pltpu.VMEM((8, BLOCK, HALF), f32),
            pltpu.VMEM((NXY, NZ, CHIP_ROWS, COLS_A), WIRE),
            pltpu.VMEM((NXY, NZ, CHIP_ROWS, COLS_A), WIRE),
            pltpu.VMEM((NZ, NXY, CHIP_ROWS, COLS_B), WIRE),
            pltpu.VMEM((NZ, NXY, CHIP_ROWS, COLS_B), WIRE),
            pltpu.VMEM((NZ, CHIP_ROWS, COLS_A), f32),
            pltpu.VMEM((NZ, CHIP_ROWS, COLS_A), f32),
            pltpu.VMEM((NXY, CHIP_ROWS, COLS_B), f32),
            pltpu.VMEM((NXY, CHIP_ROWS, COLS_B), f32),
            pltpu.VMEM((CHIP_ROWS, HALF), f32),
            pltpu.VMEM((CHIP_ROWS, HALF), f32),
            pltpu.VMEM((CORES, 4, FRAMES), bf16),
            pltpu.VMEM((NZ, CHIP_ROWS, COLS_A), bf16),
            pltpu.VMEM((NXY, CHIP_ROWS, COLS_B), bf16),
            pltpu.VMEM((CORES, NXY, NZ, CHIP_ROWS, COLS_A), bf16),
            pltpu.VMEM((CORES, NZ, NXY, CHIP_ROWS, COLS_B), bf16),
            pltpu.VMEM((FRAMES, FRAMES), f32),
            dma(8), dma(8), dma(NXY), dma(NXY), dma(NZ), dma(NZ),
            dma(NZ), dma(NZ), dma(NXY), dma(NXY), dma(2), dma(2),
            dma(NZ), dma(NZ), dma(NXY), dma(NXY),
            dma(NXY), dma(NXY), dma(NZ), dma(NZ),
            dma(NXY), dma(NXY), dma(NZ), dma(NZ),
        ],
        compiler_params=pltpu.CompilerParams(
            collective_id=0, has_side_effects=True, vmem_limit_bytes=48 * 1024 * 1024
        ),
    )(patch_features, upstream)


def on_device(patch_features, upstream):
    features = patch_features.shape[1] * lax.axis_size("grp") * lax.axis_size("dev")
    sym = grad_weights(patch_features, upstream, 1.0 / math.sqrt(features))
    return jnp.dot(sym, patch_features, preferred_element_type=jnp.float32).astype(jnp.bfloat16)


def solution(mesh):
    return jax.shard_map(
        on_device,
        mesh=mesh,
        in_specs=(P(None, ("grp", "dev")), P(("grp", "dev"), None)),
        out_specs=P(None, ("grp", "dev")),
        check_vma=False,
    )
```

```python
import functools
import math

import jax
import jax.numpy as jnp
from jax import lax
from jax.experimental import pallas as pl
from jax.experimental.pallas import tpu as pltpu
from jax.sharding import PartitionSpec as P

MESH = pl.DeviceIdType.MESH
WIRE = jnp.float32

NY, NX, NZ, NZL, NZH, CORES = 4, 4, 8, 2, 4, 2
NXY = NX * NY
CHIP_ROWS = 8
FRAMES = 1024
HALF = FRAMES // CORES
COLS_A = 384
COLS_B = HALF - COLS_A
RUN = NX * CHIP_ROWS
PAIRS = NZ // 2
FAR = NZ // 2
BLOCK = 2 * NY * RUN
TILE = 128
ROWS = 256


def comm_kernel(
    scale,
    p_hbm,
    u_hbm,
    sg,
    p_ref,
    xs,
    xr,
    sa,
    ra,
    sm,
    rm,
    sb,
    rb,
    sa2,
    ra2,
    sb2,
    rb2,
    rf,
    sf,
    hs,
    hr,
    ub,
    ga,
    gb,
    p_sem, u_in, f_sem, e_sem,
    x_send, x_recv, a_send, a_recv, m_send, m_recv, b_send, b_recv,
    a2_send, a2_recv, b2_send, b2_recv, h_sem, u_sem,
    gaz_send, gaz_recv, gbp_send, gbp_recv,
    ga1_send, ga1_recv, ga2_send, ga2_recv, gbz_send, gbz_recv,
    fa_send, fa_recv, fb_send, fb_recv,
):
    p_load = pltpu.make_async_copy(p_hbm, p_ref, p_sem.at[0])
    p_load.start()
    g = lax.axis_index("grp")
    d = lax.axis_index("dev")
    z_lo, y = lax.div(g, NY), lax.rem(g, NY)
    core = lax.rem(d, CORES)
    x = lax.rem(lax.div(d, CORES), NX)
    z_hi = lax.div(d, CORES * NX)
    z = z_hi * NZL + z_lo
    my_xy = y * NX + x
    partner = (g, d + 1 - 2 * core)
    u_load = pltpu.make_async_copy(u_hbm, ub.at[core], u_in.at[0])
    u_load.start()

    ys = [lax.rem(y + dy, NY) for dy in range(NY)]
    xs_ = [lax.rem(x + dx, NX) for dx in range(NX)]
    xy_at = []
    xy_slot = []
    for k in range(NXY):
        yt, xt = ys[k // NX], xs_[k % NX]
        xy_at.append((z_lo * NY + yt, (z_hi * NX + xt) * CORES + core))
        xy_slot.append(yt * NX + xt)

    def ring(n):
        return min(n, 4 - n)

    far_first = sorted(range(1, NXY), key=lambda k: -ring(k // NX) - ring(k % NX))

    def z_plus(dz):
        return lax.rem(z + dz, NZ)

    def at_z(dz):
        zt = z_plus(dz)
        return (
            lax.rem(zt, NZL) * NY + y,
            (lax.div(zt, NZL) * NX + x) * CORES + core,
        )

    def remote(src, dst, send, recv, to):
        return pltpu.make_async_remote_copy(
            src_ref=src, dst_ref=dst, send_sem=send, recv_sem=recv,
            device_id=to, device_id_type=MESH,
        )

    def arrived(whole, sem):
        remote(whole, whole, sem, sem, partner).wait_recv()

    def sent(whole, sem):
        remote(whole, whole, sem, sem, partner).wait_send()

    barrier = pltpu.get_barrier_semaphore()
    for dz in (4, 3, 5, 2, 6, 1, 7):
        pl.semaphore_signal(barrier, inc=1, device_id=at_z(dz), device_id_type=MESH)
    for k in reversed(range(1, NXY)):
        pl.semaphore_signal(barrier, inc=1, device_id=xy_at[k], device_id_type=MESH)
    pl.semaphore_signal(barrier, inc=1, device_id=partner, device_id_type=MESH)

    theirs = pl.multiple_of((1 - core) * HALF, HALF)
    mine = pl.multiple_of(core * HALF, HALF)

    def product(i, col0):
        runs = []
        for dz in (4 + i, 3 - i):
            zt = z_plus(dz)
            for yy in range(NY):
                row = lax.rem(zt, NZL) * (FRAMES // NZL) + yy * (FRAMES // (NZL * NY)) + lax.div(zt, NZL) * RUN
                runs.append(p_ref[pl.ds(pl.multiple_of(row, RUN), RUN), :])
        return lax.dot_general(
            jnp.concatenate(runs, axis=0),
            p_ref[pl.ds(col0, HALF), :],
            (((1,), (1,)), ((), ())),
            preferred_element_type=jnp.float32,
        )

    def x_copy(i):
        return remote(xs.at[i], xr.at[i], x_send.at[0], x_recv.at[i], partner)

    p_load.wait()
    xs[0] = product(0, theirs)
    u_load.wait()
    pl.semaphore_wait(barrier, 1 + (NXY - 1) + (NZ - 1))
    x_copy(0).start()
    u_copy = remote(ub.at[core], ub.at[core], u_sem.at[0], u_sem.at[1], partner)
    u_copy.start()

    @pl.loop(1, PAIRS)
    def _(i):
        xs[i] = product(i, theirs)
        x_copy(i).start()

    def first_axis(i, n):
        return (ys[n], xy_at[n * NX]) if i % 2 == 0 else (xs_[n], xy_at[n])

    def second_axis(i, n):
        return first_axis(i + 1, n)

    def a_copy(i, n):
        index, to = first_axis(i, n)
        return remote(sa.at[i, index], ra.at[i, n], a_send.at[0], a_recv.at[i], to)

    def m_copy(i, n):
        index, to = second_axis(i, n)
        return remote(sm.at[i, index], rm.at[i, n], m_send.at[0], m_recv.at[i], to)

    def b_copy(i, s):
        dz = 4 + i if s == 0 else 3 - i
        return remote(sb.at[i, s], rb.at[dz], b_send.at[0], b_recv.at[0], at_z(dz))

    def f_copy(k):
        return remote(sb.at[0, 0, xy_slot[k]], rf.at[k], f_sem.at[0], f_sem.at[1], xy_at[k])

    f2_copy = remote(sf.at[0], sf.at[1], f_sem.at[2], f_sem.at[3], at_z(FAR))

    for i in range(PAIRS):
        own = product(i, mine)
        x_copy(i).wait_recv()
        total = own + xr[i]
        for s in range(2):
            for m in range(NXY):
                row = (s * NXY + m) * CHIP_ROWS
                piece = total[row : row + CHIP_ROWS].astype(WIRE)
                index = (m // NX, m % NX) if i % 2 == 0 else (m % NX, m // NX)
                sa[i, index[0], index[1], s] = piece[:, :COLS_A]
                sb[i, s, m] = piece[:, COLS_A:]
        if i == 0:
            for k in far_first:
                f_copy(k).start()
        else:
            b_copy(i, 0).start()
        for n in (2, 1, 3):
            a_copy(i, n).start()
        if i < PAIRS - 1:
            b_copy(i, 1).start()

    def a2_copy(i, s):
        dz = 4 + i if s == 0 else 3 - i
        return remote(sa2.at[i, s], ra2.at[dz], a2_send.at[0], a2_recv.at[0], at_z(dz))

    def sum_first(i):
        arrived(ra.at[i, pl.ds(1, NY - 1)], a_recv.at[i])
        own = first_axis(i, 0)[0]
        for j in range(NX):
            for s in range(2):
                acc = sa[i, own, j, s].astype(jnp.float32)
                for n in range(1, NY):
                    acc = acc + ra[i, n, j, s].astype(jnp.float32)
                sm[i, j, s] = acc
        for n in (2, 1, 3):
            m_copy(i, n).start()

    def sum_second(i):
        arrived(rm.at[i, pl.ds(1, NX - 1)], m_recv.at[i])
        own = second_axis(i, 0)[0]
        for s in range(2):
            acc = sm[i, own, s]
            for n in range(1, NX):
                acc = acc + rm[i, n, s]
            sa2[i, s] = acc
        a2_copy(i, 0).start()
        if i < PAIRS - 1:
            a2_copy(i, 1).start()

    def b2_copy(k):
        return remote(
            sb2.at[xy_slot[k]], rb2.at[k], b2_send.at[0], b2_recv.at[0], xy_at[k]
        )

    sum_first(0)
    sum_first(1)
    sum_first(2)
    arrived(rf.at[pl.ds(1, NXY - 1)], f_sem.at[1])
    acc = sb[0, 0, my_xy].astype(jnp.float32)
    for k in range(1, NXY):
        acc = acc + rf[k].astype(jnp.float32)
    sf[0] = acc
    f2_copy.start()

    arrived(rb.at[pl.ds(1, NZ - 2)], b_recv.at[0])
    for m in range(NXY):
        acc = sb[PAIRS - 1, 1, m].astype(jnp.float32)
        for dz in (1, 2, 3, 5, 6, 7):
            acc = acc + rb[dz, m].astype(jnp.float32)
        sb2[m] = acc
    for k in far_first:
        b2_copy(k).start()
    sum_first(3)
    for i in range(PAIRS):
        sum_second(i)

    arrived(rb2.at[pl.ds(1, NXY - 1)], b2_recv.at[0])
    acc = sb2[my_xy]
    for k in range(1, NXY):
        acc = acc + rb2[k]
    f2_copy.wait_recv()
    hs[:, COLS_A:] = acc + sf[1]
    arrived(ra2.at[pl.ds(1, NZ - 1)], a2_recv.at[0])
    acc = sa2[PAIRS - 1, 1]
    for dz in range(1, NZ):
        acc = acc + ra2[dz]
    hs[:, :COLS_A] = acc

    h_copy = remote(hs, hr, h_sem.at[0], h_sem.at[1], partner)
    h_copy.start()
    u_copy.wait_recv()
    up = jnp.concatenate(
        [ub[0].astype(jnp.float32), ub[1].astype(jnp.float32)], axis=0
    )
    h_copy.wait_recv()

    first = core == 0
    left = jnp.where(first, hs[...], hr[...])
    right = jnp.where(first, hr[...], hs[...])
    products = jnp.concatenate([left, right], axis=1)
    row0 = z_lo * (FRAMES // NZL) + y * (FRAMES // (NZL * NY)) + z_hi * RUN + x * CHIP_ROWS
    row_ids = row0 + lax.broadcasted_iota(jnp.int32, (CHIP_ROWS, FRAMES), 0)
    col_ids = lax.broadcasted_iota(jnp.int32, (CHIP_ROWS, FRAMES), 1)
    scores = jnp.where(row_ids == col_ids, -jnp.inf, products * scale)
    row_max = jnp.max(scores, axis=1, keepdims=True)
    exponent = jnp.exp(scores - row_max)
    weights = exponent / jnp.sum(exponent, axis=1, keepdims=True)
    weighted = jnp.sum(up * weights, axis=1, keepdims=True)
    score_grad = scale * weights * (up - weighted)
    own_cols = jnp.where(first, score_grad[:, :HALF], score_grad[:, HALF:])
    own_cols = own_cols.astype(jnp.bfloat16)
    ga[core, z, y, x] = own_cols[:, :COLS_A]
    gb[core, z, y, x] = own_cols[:, COLS_A:]

    def gaz_copy(dz):
        slot = ga.at[core, z, y, x]
        return remote(slot, slot, gaz_send.at[0], gaz_recv.at[dz], at_z(dz))

    def ga1_copy(dz, n):
        slot = ga.at[core, z_plus(NZ - dz), y, x]
        to = xy_at[n] if dz % 2 == 0 else xy_at[n * NX]
        return remote(slot, slot, ga1_send.at[0], ga1_recv.at[dz], to)

    def ga2_copy(dz, n):
        if dz % 2 == 0:
            slot, to = ga.at[core, z_plus(NZ - dz), y], xy_at[n * NX]
        else:
            slot, to = ga.at[core, z_plus(NZ - dz), :, x], xy_at[n]
        return remote(slot, slot, ga2_send.at[0], ga2_recv.at[dz], to)

    def gbp_copy(k):
        slot = gb.at[core, z, y, x]
        return remote(slot, slot, gbp_send.at[0], gbp_recv.at[k // NX], xy_at[k])

    def gbz_copy(dz, dy):
        slot = gb.at[core, z, ys[(NY - dy) % NY]]
        return remote(slot, slot, gbz_send.at[0], gbz_recv.at[dz], at_z(dz))

    def fa_copy(dz):
        slot = ga.at[core, z_plus(NZ - dz)]
        return remote(slot, slot, fa_send.at[0], fa_recv.at[dz], partner)

    def fb_copy(dz):
        slot = gb.at[core, z_plus(NZ - dz)]
        return remote(slot, slot, fb_send.at[0], fb_recv.at[dz], partner)

    own_b = gb.at[core, z, y, x]
    e_copy = remote(own_b, own_b, e_sem.at[0], e_sem.at[1], at_z(FAR))

    def e2_copy(k):
        slot = gb.at[core, z_plus(FAR), y, x]
        return remote(slot, slot, e_sem.at[2], gbz_recv.at[FAR], xy_at[k])

    z_order = (3, 5, 2, 6, 1, 7)
    gaz_copy(FAR).start()
    e_copy.start()
    for dz in z_order:
        gaz_copy(dz).start()
    for k in far_first:
        gbp_copy(k).start()

    def spread_1(dz):
        if dz:
            gaz_copy(dz).wait_recv()
        for n in (2, 1, 3):
            ga1_copy(dz, n).start()

    def spread_2(dz):
        arrived(ga.at[core, z, 0, pl.ds(0, 3)], ga1_recv.at[dz])
        for n in (2, 1, 3):
            ga2_copy(dz, n).start()

    def spread_b(dy):
        count = NX if dy else NX - 1
        arrived(gb.at[core, z, 0, pl.ds(0, count)], gbp_recv.at[dy])
        for dz in z_order:
            gbz_copy(dz, dy).start()

    spread_1(0)
    spread_1(1)
    spread_1(7)
    spread_2(0)
    spread_b(0)
    spread_1(2)
    spread_1(6)
    spread_b(1)
    spread_b(3)
    spread_2(1)
    spread_2(7)
    spread_1(3)
    spread_1(5)
    spread_b(2)
    spread_1(4)
    e_copy.wait_recv()
    for k in far_first:
        e2_copy(k).start()
    spread_2(2)
    spread_2(6)
    spread_2(3)
    spread_2(5)
    spread_2(4)

    def collect(dz):
        arrived(ga.at[core, pl.ds(0, 1), pl.ds(0, 3)], ga2_recv.at[dz])
        fa_copy(dz).start()
        if dz == FAR:
            arrived(gb.at[core, pl.ds(0, 5), 0, pl.ds(0, 3)], gbz_recv.at[dz])
        elif dz:
            arrived(gb.at[core, z], gbz_recv.at[dz])
        fb_copy(dz).start()

    def place(dz):
        fa_copy(dz).wait_recv()
        fb_copy(dz).wait_recv()
        zt = z_plus(NZ - dz)
        for yy in range(NY):
            base = lax.rem(zt, NZL) * (FRAMES // NZL) + yy * (FRAMES // (NZL * NY)) + lax.div(zt, NZL) * RUN
            for xx in range(NX):
                rows = pl.ds(pl.multiple_of(base + xx * CHIP_ROWS, CHIP_ROWS), CHIP_ROWS)
                for c in range(CORES):
                    sg[rows, c * HALF : c * HALF + COLS_A] = ga[
                        c, zt, yy, xx
                    ]
                    sg[rows, c * HALF + COLS_A : (c + 1) * HALF] = gb[
                        c, zt, yy, xx
                    ]

    order = (0, 1, 7, 2, 6, 3, 5, 4)
    for n, dz in enumerate(order):
        collect(dz)
        if n:
            place(order[n - 1])
    place(order[-1])

    u_copy.wait_send()
    h_copy.wait_send()
    sent(xs, x_send.at[0])
    sent(sa.at[:, pl.ds(1, NY - 1)], a_send.at[0])
    sent(sm.at[:, pl.ds(1, NX - 1)], m_send.at[0])
    sent(rb.at[pl.ds(1, NZ - 2)], b_send.at[0])
    sent(rf.at[pl.ds(1, NXY - 1)], f_sem.at[0])
    f2_copy.wait_send()
    sent(ra2.at[pl.ds(1, NZ - 1)], a2_send.at[0])
    sent(rb2.at[pl.ds(1, NXY - 1)], b2_send.at[0])
    sent(ga.at[0, pl.ds(1, NZ - 1), 0, 0], gaz_send.at[0])
    sent(gb.at[0, pl.ds(0, 5), 0, pl.ds(0, 3)], gbp_send.at[0])
    sent(ga.at[0, pl.ds(0, 2), pl.ds(0, 3)], ga1_send.at[0])
    sent(ga.at[0, pl.ds(0, 6)], ga2_send.at[0])
    sent(gb.at[0, pl.ds(1, NZ - 2)], gbz_send.at[0])
    e_copy.wait_send()
    sent(gb.at[0, pl.ds(0, 5), 0, pl.ds(0, 3)], e_sem.at[2])
    sent(ga.at[0], fa_send.at[0])
    sent(gb.at[0], fb_send.at[0])


def sum_kernel(g_ref, p_ref, o_hbm, out, sem):
    copies = []
    for i in range(FRAMES // ROWS):
        rows = slice(i * ROWS, (i + 1) * ROWS)
        tiles = []
        for j in range(FRAMES // TILE):
            cols = slice(j * TILE, (j + 1) * TILE)
            flipped = g_ref[cols, rows].T
            total = g_ref[rows, cols].astype(jnp.float32) + flipped.astype(jnp.float32)
            tiles.append(total.astype(jnp.bfloat16))
        out[i] = jnp.dot(
            jnp.concatenate(tiles, axis=1), p_ref[...], preferred_element_type=jnp.float32
        ).astype(jnp.bfloat16)
        copy = pltpu.make_async_copy(out.at[i], o_hbm.at[pl.ds(i * ROWS, ROWS)], sem.at[i])
        copy.start()
        copies.append(copy)
    for copy in copies:
        copy.wait()


def symmetric_product(score_grad, patch_features):
    shape = patch_features.shape
    blocks = FRAMES // ROWS
    return pl.pallas_call(
        sum_kernel,
        out_shape=jax.ShapeDtypeStruct(shape, jnp.bfloat16),
        in_specs=[pl.BlockSpec(memory_space=pltpu.VMEM)] * 2,
        out_specs=pl.BlockSpec(memory_space=pltpu.HBM),
        scratch_shapes=[
            pltpu.VMEM((blocks, ROWS, shape[1]), jnp.bfloat16),
            pltpu.SemaphoreType.DMA((blocks,)),
        ],
        compiler_params=pltpu.CompilerParams(vmem_limit_bytes=24 * 1024 * 1024),
    )(score_grad, patch_features)


def grad_weights(patch_features, upstream, scale):
    dma = lambda *n: pltpu.SemaphoreType.DMA(n)
    f32, bf16 = jnp.float32, jnp.bfloat16
    return pl.pallas_call(
        functools.partial(comm_kernel, scale),
        out_shape=jax.ShapeDtypeStruct((FRAMES, FRAMES), bf16),
        in_specs=[pl.BlockSpec(memory_space=pltpu.HBM)] * 2,
        out_specs=pl.BlockSpec(memory_space=pltpu.VMEM),
        scratch_shapes=[
            pltpu.VMEM(patch_features.shape, bf16),
            pltpu.VMEM((PAIRS, BLOCK, HALF), f32),
            pltpu.VMEM((PAIRS, BLOCK, HALF), f32),
            pltpu.VMEM((PAIRS, NY, NX, 2, CHIP_ROWS, COLS_A), WIRE),
            pltpu.VMEM((PAIRS, NY, NX, 2, CHIP_ROWS, COLS_A), WIRE),
            pltpu.VMEM((PAIRS, NX, 2, CHIP_ROWS, COLS_A), f32),
            pltpu.VMEM((PAIRS, NX, 2, CHIP_ROWS, COLS_A), f32),
            pltpu.VMEM((PAIRS, 2, NXY, CHIP_ROWS, COLS_B), WIRE),
            pltpu.VMEM((NZ, NXY, CHIP_ROWS, COLS_B), WIRE),
            pltpu.VMEM((PAIRS, 2, CHIP_ROWS, COLS_A), f32),
            pltpu.VMEM((NZ, CHIP_ROWS, COLS_A), f32),
            pltpu.VMEM((NXY, CHIP_ROWS, COLS_B), f32),
            pltpu.VMEM((NXY, CHIP_ROWS, COLS_B), f32),
            pltpu.VMEM((NXY, CHIP_ROWS, COLS_B), WIRE),
            pltpu.VMEM((2, CHIP_ROWS, COLS_B), f32),
            pltpu.VMEM((CHIP_ROWS, HALF), f32),
            pltpu.VMEM((CHIP_ROWS, HALF), f32),
            pltpu.VMEM((CORES, 4, FRAMES), bf16),
            pltpu.VMEM((CORES, NZ, NY, NX, CHIP_ROWS, COLS_A), bf16),
            pltpu.VMEM((CORES, NZ, NY, NX, CHIP_ROWS, COLS_B), bf16),
            dma(1), dma(1), dma(4), dma(3),
            dma(1), dma(PAIRS), dma(1), dma(PAIRS), dma(1), dma(PAIRS), dma(1), dma(1),
            dma(1), dma(1), dma(1), dma(1), dma(2), dma(2),
            dma(1), dma(NZ), dma(1), dma(NY),
            dma(1), dma(NZ), dma(1), dma(NZ), dma(1), dma(NZ),
            dma(1), dma(NZ), dma(1), dma(NZ),
        ],
        compiler_params=pltpu.CompilerParams(
            collective_id=0, has_side_effects=True, vmem_limit_bytes=40 * 1024 * 1024
        ),
    )(pltpu.with_memory_space_constraint(patch_features, pltpu.HBM), pltpu.with_memory_space_constraint(upstream, pltpu.HBM))


def on_device(patch_features, upstream):
    features = patch_features.shape[1] * lax.axis_size("grp") * lax.axis_size("dev")
    score_grad = grad_weights(patch_features, upstream, 1.0 / math.sqrt(features))
    return symmetric_product(score_grad, patch_features)


def solution(mesh):
    return jax.shard_map(
        on_device,
        mesh=mesh,
        in_specs=(P(None, ("grp", "dev")), P(("grp", "dev"), None)),
        out_specs=P(None, ("grp", "dev")),
        check_vma=False,
    )
```
